256 devices in a mesh: grp: 8 (over y, core), node: 32 (over z, x).
Axes of the slice: x: 4, y: 4, z: 8, core: 2. Of those that a mesh axis runs over, the one named last changes fastest.
Arguments:
- excitation: float32 [128, 262144], P(None, ('grp', 'node')), may hold values from -6 to 6
- points: float32 [3, 262144], P(None, ('grp', 'node')), may hold values from -5 to 5
- near_mask: int32 [256, 2], P(('grp', 'node')), may hold values from 0 to 1, as said below
- bit_order: int32 [3], replicated, may hold values from 0 to 2, as said below
- compress: float32 [262144, 256], P(('grp', 'node')), may hold values from -0.1875 to 0.1875
- level_self: float32 [3, 65536, 256], P(None, ('grp', 'node')), may hold values from -0.25 to 0.25
- level_partner: float32 [3, 65536, 256], P(None, ('grp', 'node')), may hold values from -0.25 to 0.25
- expand: float32 [65536, 8192], P(('grp', 'node')), may hold values from -0.375 to 0.375
Outputs:
- field: float32 [128, 262144], P(None, ('grp', 'node'))
The draws below stay inside these ranges and needn't reach their ends.
Inputs may be any that keep to these rules, and one draw needn't show every extreme that they name: near_mask[b, 0] is 0 when b is the first cluster of its group and near_mask[b, 1] is 0 when b is the last; otherwise each entry is 0 or 1. `bit_order`: the entries are distinct bits of a node index; each of 0 to 2 appears once.
All inputs are finite; a program needn't handle non-finite values.
Results may differ from the reference program's by a relative error of at most 0.0001.
Values sent between devices are 32-bit elements; how exact they have to be, the bound alone decides.
A program may use at most 64 MiB of HBM per device.

```python
import math
import jax
import jax.numpy as jnp
from jax import lax

BLOCK = 1024
RANK = 256
COLS = 128
LEVELS = 3
BLOCKS = 256
ROWS = 262144
GROUP_ROWS = 8192
N_GRP = 8
N_NODE = 32


def draw_near_mask(key, part):
    flags = jax.random.randint(jax.random.fold_in(key, 11), (BLOCKS, 2), 0, 2).astype(jnp.int32)
    position = jnp.arange(BLOCKS, dtype=jnp.int32) % N_NODE
    first = (position != 0).astype(jnp.int32)
    last = (position != N_NODE - 1).astype(jnp.int32)
    return jnp.stack([flags[:, 0] * first, flags[:, 1] * last], axis=1)


def draw_bit_order(key, part):
    return jax.random.permutation(jax.random.fold_in(key, 23), LEVELS).astype(jnp.int32)


def block_levels(key, extent, cuts, least, largest):
    level = 1.0
    for axis_at, parts in cuts:
        steps = jax.random.uniform(jax.random.fold_in(jax.random.fold_in(key, 6), axis_at), (parts,), jnp.float32, least / len(cuts), largest / len(cuts))
        level = level * jnp.repeat(jnp.exp(steps), extent[axis_at] // parts).reshape((-1,) + (1,) * (len(extent) - 1 - axis_at))
    return level


def gaussian(key, shape, width, most, split=(), held_as=jnp.bfloat16):
    factor_of = block_levels(key, shape, split, -0.22, 0.18) if split else 1.0
    result = jax.random.normal(key, shape, jnp.float32) * width * factor_of
    return jnp.minimum(jnp.maximum(result, -most), most).astype(held_as)


def setup_inputs(seed: int = 0) -> dict:
    key_of = jax.random.split(jax.random.key(seed), 9)
    excitation = gaussian(key_of[0], (COLS, ROWS), 1.0, 6.0, ((1, 256),), jnp.float32)
    points = gaussian(key_of[1], (3, ROWS), 1.0, 5.0, ((1, 256),), jnp.float32)
    near_mask = draw_near_mask(jax.random.fold_in(key_of[8], 71), 0)
    bit_order = draw_bit_order(jax.random.fold_in(key_of[8], 71), 0)
    compress = gaussian(key_of[4], (ROWS, RANK), BLOCK ** -0.5, 0.1875, ((0, 256),), jnp.float32)
    level_self = gaussian(key_of[5], (LEVELS, BLOCKS * RANK, RANK), (2 * RANK) ** -0.5, 0.25, ((1, 256),), jnp.float32)
    level_partner = gaussian(key_of[6], (LEVELS, BLOCKS * RANK, RANK), (2 * RANK) ** -0.5, 0.25, ((1, 256),), jnp.float32)
    expand = gaussian(key_of[7], (BLOCKS * RANK, GROUP_ROWS), RANK ** -0.5, 0.375, ((0, 256),), jnp.float32)
    return dict(excitation=excitation, points=points, near_mask=near_mask, bit_order=bit_order, compress=compress, level_self=level_self, level_partner=level_partner, expand=expand)


HIGH = lax.Precision.HIGHEST
SOFTEN = 0.01

def kernel_block(sources, targets):
    dist_sq = (sources[0][:, None] - targets[0][None, :]) ** 2
    dist_sq = dist_sq + (sources[1][:, None] - targets[1][None, :]) ** 2
    dist_sq = dist_sq + (sources[2][:, None] - targets[2][None, :]) ** 2
    return lax.rsqrt(dist_sq + SOFTEN) * (1.0 / math.sqrt(sources.shape[1]))

def reference(excitation, points, near_mask, bit_order, compress, level_self, level_partner, expand):
    blocked = excitation.reshape(COLS, BLOCKS, BLOCK).transpose(1, 0, 2)
    coords = points.reshape(3, BLOCKS, BLOCK).transpose(1, 0, 2)
    comp = compress.reshape(BLOCKS, BLOCK, RANK)
    state = jnp.einsum('bcr,brk->bck', blocked, comp, precision=HIGH)
    selfs = level_self.reshape(LEVELS, BLOCKS, RANK, RANK)
    others = level_partner.reshape(LEVELS, BLOCKS, RANK, RANK)
    labels = jnp.arange(BLOCKS, dtype=jnp.int32)
    for level in range(LEVELS):
        partner = jnp.bitwise_xor(labels, jnp.left_shift(jnp.int32(1), bit_order[level]).astype(jnp.int32))
        moved = jnp.take(state, partner, axis=0)
        state = jnp.einsum('bck,bkr->bcr', state, selfs[level], precision=HIGH) + jnp.einsum('bck,bkr->bcr', moved, others[level], precision=HIGH)
    grouped = state.reshape(N_GRP, N_NODE, COLS, RANK)
    maps = expand.reshape(N_GRP, N_NODE, RANK, N_GRP, BLOCK)
    far = jnp.einsum('gncr,gnrhk->hnck', grouped, maps, precision=HIGH).reshape(BLOCKS, COLS, BLOCK)
    flags = near_mask.astype(jnp.float32)
    before_x = jnp.roll(blocked, 1, axis=0)
    after_x = jnp.roll(blocked, -1, axis=0)
    before_p = jnp.roll(coords, 1, axis=0)
    after_p = jnp.roll(coords, -1, axis=0)

    def near_one(items):
        own_x, own_p, left_x, left_p, right_x, right_p, flag = items
        total = jnp.dot(own_x, kernel_block(own_p, own_p), precision=HIGH)
        total = total + flag[0] * jnp.dot(left_x, kernel_block(left_p, own_p), precision=HIGH)
        total = total + flag[1] * jnp.dot(right_x, kernel_block(right_p, own_p), precision=HIGH)
        return total
    near = lax.map(near_one, (blocked, coords, before_x, before_p, after_x, after_p, flags))
    return (far + near).transpose(1, 0, 2).reshape(COLS, ROWS)
```

```python
import functools
import itertools

import jax
import jax.numpy as jnp
from jax import lax
from jax.experimental import pallas as pl
from jax.experimental.pallas import tpu as pltpu
from jax.sharding import PartitionSpec as P

F32 = jnp.float32
BF16 = jnp.bfloat16
MESH = pl.DeviceIdType.MESH
SOFTEN = 0.01

PARTS = 4
AWAY = (2, 3, 1, 0)


def split(value):
    high = value.astype(BF16)
    return high, (value - high.astype(F32)).astype(BF16)


def product(left, right_high, right_low):
    rows = left.shape[0] // 2
    both = jnp.dot(left, right_high, preferred_element_type=F32)
    rest = jnp.dot(left[:rows], right_low, preferred_element_type=F32)
    return both[:rows] + both[rows:] + rest


def stacked(value):
    return jnp.concatenate(split(value), axis=0)


def remote(source, target, sends, receives, device):
    return pltpu.make_async_remote_copy(
        src_ref=source,
        dst_ref=target,
        send_sem=sends,
        recv_sem=receives,
        device_id=device,
        device_id_type=MESH,
    )


def kernel(
    bits,
    sizes,
    x_hbm,
    points_hbm,
    mask,
    compress_hbm,
    self_hbm,
    partner_hbm,
    expand_hbm,
    out_hbm,
    x,
    points,
    columns,
    compress,
    weights,
    weights_high,
    weights_low,
    expand,
    expand_high,
    expand_low,
    g_high,
    g_low,
    x_both,
    near,
    state,
    moved,
    peer_state,
    share,
    first,
    straight,
    relayed,
    out,
    load_sem,
    expand_sem,
    out_sem,
    level_sems,
    peer_sems,
    peer_expand_sems,
    points_sems,
    x_sems,
    first_sems,
    straight_sems,
    relayed_sems,
):
    n_grp, n_node = sizes
    levels = len(bits)
    cols, block = x_hbm.shape
    rank = compress_hbm.shape[1]
    part = cols // PARTS
    half = block // 2
    ring = n_grp // 2

    grp, node = lax.axis_index("grp"), lax.axis_index("node")
    y, core = lax.div(grp, 2), lax.rem(grp, 2)

    def along(step):
        return (lax.rem(y + step, ring) * 2 + core, node)

    up, down = along(1), along(ring - 1)
    peer = (grp + 1 - 2 * core, node)
    after = (grp, lax.rem(node + 1, n_node))
    before = (grp, lax.rem(node + n_node - 1, n_node))

    def partner(bit):
        apart = 1 << bit
        return (grp, node + apart * (1 - 2 * lax.rem(lax.div(node, apart), 2)))

    partners = [partner(bit) for bit in bits]

    loads = [
        pltpu.make_async_copy(x_hbm, x.at[0], load_sem.at[0]),
        pltpu.make_async_copy(compress_hbm, compress, load_sem.at[1]),
        pltpu.make_async_copy(points_hbm, points.at[0], load_sem.at[2]),
        pltpu.make_async_copy(self_hbm, weights.at[0], load_sem.at[3]),
        pltpu.make_async_copy(partner_hbm, weights.at[1], load_sem.at[4]),
    ]
    for load in loads:
        load.start()

    barrier = pltpu.get_barrier_semaphore()
    everyone = partners + [peer, up, down, before, after]
    for device in everyone:
        pl.semaphore_signal(barrier, inc=1, device_id=device, device_id_type=MESH)

    def expand_columns(slot, of_core):
        target = lax.rem(y + AWAY[slot], ring) * 2 + of_core
        return expand_hbm.at[:, pl.ds(pl.multiple_of(target * block, block), block)]

    own_expand = [
        pltpu.make_async_copy(expand_columns(slot, core), expand.at[slot, 0], expand_sem.at[slot])
        for slot in range(ring)
    ]
    for copy in own_expand:
        copy.start()

    loads[0].wait()
    x_both[0] = stacked(x[0])
    loads[1].wait()
    state[0] = product(x_both[0], *split(compress[...]))

    pl.semaphore_wait(barrier, len(everyone))

    def level_copy(level, chunk):
        rows = pl.ds(pl.multiple_of(chunk * part, part), part)
        return remote(
            state.at[level, rows],
            moved.at[level, rows],
            level_sems.at[0, level, chunk],
            level_sems.at[1, level, chunk],
            partners[level],
        )

    for chunk in range(PARTS):
        level_copy(0, chunk).start()

    loads[2].wait()
    to_after = remote(points.at[0], points.at[1], points_sems.at[0, 0], points_sems.at[1, 0], after)
    to_before = remote(points.at[0], points.at[2], points_sems.at[0, 1], points_sems.at[1, 1], before)
    to_after.start()
    to_before.start()

    peer_expand = [
        remote(
            expand_columns(slot, 1 - core),
            expand.at[slot, 1],
            peer_expand_sems.at[0, slot],
            peer_expand_sems.at[1, slot],
            peer,
        )
        for slot in range(ring)
    ]
    for copy in peer_expand:
        copy.start()

    for which in range(2):
        loads[3 + which].wait()
    for level in range(levels):
        for which in range(2):
            high, low = split(weights[which, level])
            weights_high[which, level] = high
            weights_low[which, level] = low

    def turn(which):
        padded = jnp.concatenate([points[which] * 32.0, jnp.zeros((5, block), F32)], axis=0)
        columns[pl.ds(which * block, block), :] = padded.T

    tall = 16
    wide = block // tall

    def g_rows(index):
        rows = pl.ds(pl.multiple_of(index * tall, tall), tall)
        total = None
        for axis in range(3):
            apart = columns[rows, axis : axis + 1] - points[0, axis : axis + 1, :] * 32.0
            total = apart * apart if total is None else total + apart * apart
        high, low = split(lax.rsqrt(total + SOFTEN * 1024.0))
        g_high[rows, :] = high
        g_low[rows, :] = low

    def g_span(low, high):
        def body(index, carry):
            g_rows(index)
            return carry

        lax.fori_loop(low, high, body, 0)

    turn(0)
    g_span(0, wide)

    def level_step(level, chunk):
        rows = pl.ds(pl.multiple_of(chunk * part, part), part)
        own = product(stacked(state[level, rows]), weights_high[0, level], weights_low[0, level])
        level_copy(level, chunk).wait_recv()
        came = product(stacked(moved[level, rows]), weights_high[1, level], weights_low[1, level])
        state[level + 1, rows] = own + came

    for level in range(levels - 1):

        def level_body(chunk, carry, level=level):
            level_step(level, chunk)
            level_copy(level + 1, chunk).start()
            return carry

        lax.fori_loop(0, PARTS, level_body, 0)
        if level == 0:
            to_after.wait_recv()
            to_before.wait_recv()
            turn(1)
            turn(2)

    x_after = remote(x.at[0], x.at[1], x_sems.at[0, 0], x_sems.at[1, 0], after)
    x_before = remote(x.at[0], x.at[2], x_sems.at[0, 1], x_sems.at[1, 1], before)
    x_after.start()
    x_before.start()

    for slot in range(ring):
        own_expand[slot].wait()
        peer_expand[slot].wait_recv()

        def convert(index, carry, slot=slot):
            rows = pl.ds(pl.multiple_of(index * 32, 32), 32)
            for which in range(2):
                high, low = split(expand[slot, which, rows, :])
                expand_high[slot, which, rows, :] = high
                expand_low[slot, which, rows, :] = low
            return carry

        lax.fori_loop(0, rank // 32, convert, 0)

    def peer_copy(chunk):
        rows = pl.ds(pl.multiple_of(chunk * part, part), part)
        return remote(
            state.at[levels, rows],
            peer_state.at[rows],
            peer_sems.at[0, chunk],
            peer_sems.at[1, chunk],
            peer,
        )

    def first_copy(chunk, side):
        return remote(
            share.at[chunk, 0, side],
            first.at[chunk, side],
            first_sems.at[0, chunk, side],
            first_sems.at[1, chunk, side],
            (down, up)[side],
        )

    def straight_copy(chunk, side):
        return remote(
            share.at[chunk, 1 + side, 1 - side],
            straight.at[chunk, side],
            straight_sems.at[0, chunk, side],
            straight_sems.at[1, chunk, side],
            (down, up)[side],
        )

    def relayed_copy(chunk, side):
        return remote(
            share.at[chunk, 1 + side, side],
            relayed.at[chunk, side],
            relayed_sems.at[0, chunk, side],
            relayed_sems.at[1, chunk, side],
            (down, up)[side],
        )

    def far_step(chunk):
        rows = pl.ds(pl.multiple_of(chunk * part, part), part)
        own = stacked(state[levels, rows])
        peer_copy(chunk).wait_recv()
        other = stacked(peer_state[rows])
        for slot in range(ring):
            for side in range(2):
                span = pl.ds(side * half, half)
                share[chunk, slot, side] = product(
                    own, expand_high[slot, 0, :, span], expand_low[slot, 0, :, span]
                ) + product(other, expand_high[slot, 1, :, span], expand_low[slot, 1, :, span])
            if slot == 0:
                first_copy(chunk, 0).start()
                first_copy(chunk, 1).start()
            if slot == 1:
                straight_copy(chunk, 0).start()
            if slot == 2:
                straight_copy(chunk, 1).start()

    def relay_step(chunk):
        for side in range(2):
            first_copy(chunk, side).wait_recv()
            share[chunk, 1 + side, side] = share[chunk, 1 + side, side] + first[chunk, side]
            relayed_copy(chunk, side).start()

    turns = PARTS + 2
    each = -(-2 * wide // turns)

    def main_body(step, carry):
        @pl.when(step < PARTS)
        def _():
            level_step(levels - 1, step)
            peer_copy(step).start()

        @pl.when(jnp.logical_and(step >= 1, step < PARTS + 1))
        def _():
            far_step(step - 1)

        @pl.when(step >= 2)
        def _():
            relay_step(step - 2)

        g_span(wide + step * each, jnp.minimum(wide + (step + 1) * each, 3 * wide))
        return carry

    lax.fori_loop(0, turns, main_body, 0)

    for which in range(3):
        if which == 1:
            x_after.wait_recv()
        if which == 2:
            x_before.wait_recv()
        if which:
            x_both[which] = stacked(x[which] * mask[0, which - 1].astype(F32))

        def near_body(index, carry, which=which):
            span = pl.ds(pl.multiple_of(index * 256, 256), 256)
            rows = pl.ds(which * block, block)
            term = product(x_both[which], g_high[rows, span], g_low[rows, span])
            near[:, span] = term if which == 0 else near[:, span] + term
            return carry

        lax.fori_loop(0, block // 256, near_body, 0)

    def out_copy(chunk):
        rows = pl.ds(pl.multiple_of(chunk * part, part), part)
        return pltpu.make_async_copy(out.at[rows], out_hbm.at[rows], out_sem.at[chunk])

    def final_body(chunk, carry):
        rows = pl.ds(pl.multiple_of(chunk * part, part), part)
        for side in range(2):
            straight_copy(chunk, 1 - side).wait_recv()
            relayed_copy(chunk, side).wait_recv()
            span = pl.ds(side * half, half)
            out[rows, span] = (
                near[rows, span]
                + share[chunk, 3, side]
                + straight[chunk, 1 - side]
                + relayed[chunk, side]
            )
        out_copy(chunk).start()
        return carry

    lax.fori_loop(0, PARTS, final_body, 0)

    def drain(chunk, carry):
        for level in range(levels):
            level_copy(level, chunk).wait_send()
        peer_copy(chunk).wait_send()
        for side in range(2):
            first_copy(chunk, side).wait_send()
            straight_copy(chunk, side).wait_send()
            relayed_copy(chunk, side).wait_send()
        out_copy(chunk).wait()
        return carry

    lax.fori_loop(0, PARTS, drain, 0)
    for copy in [to_after, to_before, x_after, x_before] + peer_expand:
        copy.wait_send()


def solution(mesh):
    sizes = (mesh.shape["grp"], mesh.shape["node"])

    def shards(excitation, points, near_mask, bit_order, compress, level_self, level_partner, expand):
        cols, block = excitation.shape
        rank = compress.shape[1]
        levels = level_self.shape[0]
        part = cols // PARTS
        half = block // 2
        ring = sizes[0] // 2
        hbm = pl.BlockSpec(memory_space=pltpu.HBM)
        dma = pltpu.SemaphoreType.DMA

        def call(bits, number):
            return pl.pallas_call(
                functools.partial(kernel, bits, sizes),
                out_shape=jax.ShapeDtypeStruct((cols, block), F32),
                in_specs=[hbm, hbm, pl.BlockSpec(memory_space=pltpu.SMEM), hbm, hbm, hbm, hbm],
                out_specs=hbm,
                scratch_shapes=[
                    pltpu.VMEM((3, cols, block), F32),
                    pltpu.VMEM((3, 3, block), F32),
                    pltpu.VMEM((3 * block, 8), F32),
                    pltpu.VMEM((block, rank), F32),
                    pltpu.VMEM((2, levels, rank, rank), F32),
                    pltpu.VMEM((2, levels, rank, rank), BF16),
                    pltpu.VMEM((2, levels, rank, rank), BF16),
                    pltpu.VMEM((ring, 2, rank, block), F32),
                    pltpu.VMEM((ring, 2, rank, block), BF16),
                    pltpu.VMEM((ring, 2, rank, block), BF16),
                    pltpu.VMEM((3 * block, block), BF16),
                    pltpu.VMEM((3 * block, block), BF16),
                    pltpu.VMEM((3, 2 * cols, block), BF16),
                    pltpu.VMEM((cols, block), F32),
                    pltpu.VMEM((levels + 1, cols, rank), F32),
                    pltpu.VMEM((levels, cols, rank), F32),
                    pltpu.VMEM((cols, rank), F32),
                    pltpu.VMEM((PARTS, ring, 2, part, half), F32),
                    pltpu.VMEM((PARTS, 2, part, half), F32),
                    pltpu.VMEM((PARTS, 2, part, half), F32),
                    pltpu.VMEM((PARTS, 2, part, half), F32),
                    pltpu.VMEM((cols, block), F32),
                    dma((5,)),
                    dma((ring,)),
                    dma((PARTS,)),
                    dma((2, levels, PARTS)),
                    dma((2, PARTS)),
                    dma((2, ring)),
                    dma((2, 2)),
                    dma((2, 2)),
                    dma((2, PARTS, 2)),
                    dma((2, PARTS, 2)),
                    dma((2, PARTS, 2)),
                ],
                compiler_params=pltpu.CompilerParams(
                    collective_id=number, has_side_effects=True, vmem_limit_bytes=62 << 20
                ),
                name=f"far_near_{number}",
            )

        orders = list(itertools.permutations(range(levels)))
        branches = [call(bits, number) for number, bits in enumerate(orders)]
        which = bit_order[0] * 2 + (bit_order[1] > bit_order[2]).astype(jnp.int32)
        return lax.switch(
            which,
            branches,
            excitation,
            points,
            near_mask,
            compress,
            level_self,
            level_partner,
            expand,
        )

    return jax.shard_map(
        shards,
        mesh=mesh,
        in_specs=(
            P(None, ("grp", "node")),
            P(None, ("grp", "node")),
            P(("grp", "node"), None),
            P(),
            P(("grp", "node"), None),
            P(None, ("grp", "node"), None),
            P(None, ("grp", "node"), None),
            P(("grp", "node"), None),
        ),
        out_specs=P(None, ("grp", "node")),
        check_vma=False,
    )
```

```python
import functools
import itertools

import jax
import jax.numpy as jnp
from jax import lax
from jax.experimental import pallas as pl
from jax.experimental.pallas import tpu as pltpu
from jax.sharding import PartitionSpec as P

F32 = jnp.float32
BF16 = jnp.bfloat16
MESH = pl.DeviceIdType.MESH
SOFTEN = 0.01

TALL = 64
FILLS = (10, 20, 25, 48)
PARTS = 4
AWAY = (2, 3, 1, 0)


def split(value):
    high = value.astype(BF16)
    return high, (value - high.astype(F32)).astype(BF16)


def product(left, right_high, right_low):
    rows = left.shape[0] // 2
    both = jnp.dot(left, right_high, preferred_element_type=F32)
    rest = jnp.dot(left[:rows], right_low, preferred_element_type=F32)
    return both[:rows] + both[rows:] + rest


def stacked(value):
    return jnp.concatenate(split(value), axis=0)


def remote(source, target, sends, receives, device):
    return pltpu.make_async_remote_copy(
        src_ref=source,
        dst_ref=target,
        send_sem=sends,
        recv_sem=receives,
        device_id=device,
        device_id_type=MESH,
    )


def kernel(
    bits,
    sizes,
    x_hbm,
    points_hbm,
    mask_hbm,
    compress_hbm,
    self_hbm,
    partner_hbm,
    expand_hbm,
    out,
    mask,
    x,
    points,
    columns,
    spread,
    compress,
    weights,
    weights_high,
    weights_low,
    expand,
    expand_high,
    expand_low,
    g_high,
    g_low,
    x_both,
    near,
    state,
    moved,
    peer_state,
    share,
    first,
    straight,
    relayed,
    load_sem,
    expand_sem,
    sent_sems,
    level_sems,
    peer_sems,
    peer_expand_sems,
    points_sems,
    x_sems,
    first_sems,
    straight_sem,
    relayed_sems,
):
    n_grp, n_node = sizes
    levels = len(bits)
    cols, block = x_hbm.shape
    rank = compress_hbm.shape[1]
    part = cols // PARTS
    half = block // 2
    ring = n_grp // 2

    grp, node = lax.axis_index("grp"), lax.axis_index("node")
    y, core = lax.div(grp, 2), lax.rem(grp, 2)

    def along(step):
        return (lax.rem(y + step, ring) * 2 + core, node)

    up, down = along(1), along(ring - 1)
    peer = (grp + 1 - 2 * core, node)
    after, before = (grp, node + 1), (grp, node - 1)

    def partner(bit):
        apart = 1 << bit
        return (grp, node + apart * (1 - 2 * lax.rem(lax.div(node, apart), 2)))

    partners = [partner(bit) for bit in bits]
    has_before, has_after = node > 0, node < n_node - 1

    loads = [
        pltpu.make_async_copy(x_hbm, x.at[0], load_sem.at[0]),
        pltpu.make_async_copy(compress_hbm, compress, load_sem.at[1]),
        pltpu.make_async_copy(points_hbm, points.at[0], load_sem.at[2]),
        pltpu.make_async_copy(mask_hbm, mask, load_sem.at[3]),
        pltpu.make_async_copy(self_hbm, weights.at[0], load_sem.at[4]),
        pltpu.make_async_copy(partner_hbm, weights.at[1], load_sem.at[4]),
    ]
    for load in loads[:2]:
        load.start()

    barrier = pltpu.get_barrier_semaphore()

    def greet(device):
        pl.semaphore_signal(barrier, inc=1, device_id=device, device_id_type=MESH)

    everyone = partners + [peer, up, down]
    for device in everyone:
        greet(device)

    @pl.when(has_before)
    def _():
        greet(before)

    @pl.when(has_after)
    def _():
        greet(after)

    for load in loads[2:]:
        load.start()

    def expand_columns(slot, of_core):
        target = lax.rem(y + AWAY[slot], ring) * 2 + of_core
        return expand_hbm.at[:, pl.ds(pl.multiple_of(target * block, block), block)]

    own_expand = [
        pltpu.make_async_copy(expand_columns(slot, core), expand.at[slot, pl.ds(0, rank)], expand_sem)
        for slot in range(ring)
    ]

    with jax.named_scope("load_x"):
        loads[0].wait()
    with jax.named_scope("split_x"):
        x_both[0] = stacked(x[0])
    with jax.named_scope("load_c"):
        loads[1].wait()
        for copy in own_expand:
            copy.start()
    with jax.named_scope("compress"):
        state[0] = product(x_both[0], *split(compress[...]))

    with jax.named_scope("barrier"):
        pl.semaphore_wait(barrier, len(everyone) + has_before.astype(jnp.int32) + has_after.astype(jnp.int32))

    def level_copy(level, chunk):
        rows = pl.ds(pl.multiple_of(chunk * part, part), part)
        return remote(
            state.at[level, rows],
            moved.at[level, rows],
            sent_sems.at[level],
            level_sems.at[level, chunk],
            partners[level],
        )

    for chunk in range(PARTS):
        level_copy(0, chunk).start()

    loads[2].wait()
    to_after = remote(points.at[0], points.at[1], points_sems.at[0, 0], points_sems.at[1, 0], after)
    to_before = remote(points.at[0], points.at[2], points_sems.at[0, 1], points_sems.at[1, 1], before)

    @pl.when(has_after)
    def _():
        to_after.start()

    @pl.when(has_before)
    def _():
        to_before.start()

    @pl.when(jnp.logical_not(has_before))
    def _():
        points[1] = jnp.zeros_like(points[1])
        x[1] = jnp.zeros_like(x[1])

    @pl.when(jnp.logical_not(has_after))
    def _():
        points[2] = jnp.zeros_like(points[2])
        x[2] = jnp.zeros_like(x[2])

    peer_expand = [
        remote(
            expand_columns(slot, 1 - core),
            expand.at[slot, pl.ds(rank, rank)],
            peer_expand_sems.at[0],
            peer_expand_sems.at[1],
            peer,
        )
        for slot in range(ring)
    ]
    for copy in peer_expand:
        copy.start()

    with jax.named_scope("split_w"):
        loads[3].wait()
        pltpu.make_async_copy(weights, weights, load_sem.at[4]).wait()
        for level in range(levels):
            for which in range(2):
                high, low = split(weights[which, level])
                weights_high[which, level] = high
                weights_low[which, level] = low

    def turn(which):
        padded = jnp.concatenate([points[which] * 32.0, jnp.zeros((5, block), F32)], axis=0)
        columns[pl.ds(which * block, block), :] = padded.T

    def g_rows(index):
        for piece in range(TALL // 16):
            rows = pl.ds(pl.multiple_of(index * TALL + piece * 16, 16), 16)
            column = columns[rows, :]
            for side in range(2):
                span = pl.ds(side * half, half)
                total = None
                for axis in range(3):
                    source = jnp.broadcast_to(column[:, axis : axis + 1], (16, half))
                    target = jnp.concatenate([spread[axis, :, span]] * 2, axis=0)
                    apart = source - target
                    total = apart * apart if total is None else total + apart * apart
                high, low = split(lax.rsqrt(total + SOFTEN * 1024.0))
                g_high[rows, span] = high
                g_low[rows, span] = low

    wide = block // TALL

    def g_span(low, high):
        def body(index, carry):
            g_rows(index)
            return carry

        lax.fori_loop(low, high, body, 0)

    def near_part(which):
        def near_body(index, carry):
            span = pl.ds(pl.multiple_of(index * 512, 512), 512)
            rows = pl.ds(which * block, block)
            term = product(x_both[which], g_high[rows, span], g_low[rows, span])
            near[:, span] = term if which == 0 else near[:, span] + term
            return carry

        with jax.named_scope(f"near{which}"):
            lax.fori_loop(0, block // 512, near_body, 0)

    with jax.named_scope("turn0"):
        for axis in range(3):
            spread[axis] = jnp.broadcast_to(points[0, axis : axis + 1, :] * 32.0, (8, block))
        turn(0)
    with jax.named_scope("g_own"):
        g_span(0, FILLS[0])

    def level_step(level, chunk):
        rows = pl.ds(pl.multiple_of(chunk * part, part), part)
        with jax.named_scope(f"own{level}"):
            own = product(stacked(state[level, rows]), weights_high[0, level], weights_low[0, level])
        with jax.named_scope(f"wait{level}"):
            level_copy(level, chunk).wait_recv()
        with jax.named_scope(f"came{level}"):
            came = product(stacked(moved[level, rows]), weights_high[1, level], weights_low[1, level])
            state[level + 1, rows] = own + came

    for level in range(levels - 1):

        def level_body(chunk, carry, level=level):
            level_step(level, chunk)
            level_copy(level + 1, chunk).start()
            return carry

        lax.fori_loop(0, PARTS, level_body, 0)
        if level == 0:
            with jax.named_scope("turn12"):
                pl.when(has_before)(to_after.wait_recv)
                pl.when(has_after)(to_before.wait_recv)
                turn(1)
                turn(2)
            with jax.named_scope("g_1"):
                g_span(FILLS[0], FILLS[1])

    x_after = remote(x.at[0], x.at[1], x_sems.at[0, 0], x_sems.at[1, 0], after)
    x_before = remote(x.at[0], x.at[2], x_sems.at[0, 1], x_sems.at[1, 1], before)
    pl.when(has_after)(x_after.start)
    pl.when(has_before)(x_before.start)

    whole_expand = remote(
        expand.at[:, pl.ds(0, rank)],
        expand.at[:, pl.ds(rank, rank)],
        peer_expand_sems.at[0],
        peer_expand_sems.at[1],
        peer,
    )
    with jax.named_scope("wait_e"):
        pltpu.make_async_copy(
            expand.at[:, pl.ds(0, rank)], expand.at[:, pl.ds(0, rank)], expand_sem
        ).wait()
        whole_expand.wait_recv()
    for slot in range(ring):

        def convert(index, carry, slot=slot):
            rows = pl.ds(pl.multiple_of(index * 32, 32), 32)
            high, low = split(expand[slot, rows, :])
            expand_high[slot, rows, :] = high
            expand_low[slot, rows, :] = low
            return carry

        with jax.named_scope("convert"):
            lax.fori_loop(0, rank // 16, convert, 0)

    with jax.named_scope("g_2"):
        g_span(FILLS[1], FILLS[2])

    def peer_copy(chunk):
        rows = pl.ds(pl.multiple_of(chunk * part, part), part)
        return remote(
            state.at[levels, rows],
            peer_state.at[rows],
            sent_sems.at[levels],
            peer_sems.at[chunk],
            peer,
        )

    def first_copy(chunk, side):
        return remote(
            share.at[chunk, 0, side],
            first.at[chunk, side],
            sent_sems.at[levels + 1],
            first_sems.at[chunk, side],
            (down, up)[side],
        )

    def straight_copy(chunk, side):
        return remote(
            share.at[chunk, 1 + side, 1 - side],
            straight.at[chunk, side],
            sent_sems.at[levels + 1],
            straight_sem,
            (down, up)[side],
        )

    def relayed_copy(chunk, side):
        return remote(
            share.at[chunk, 1 + side, side],
            relayed.at[chunk, side],
            sent_sems.at[levels + 1],
            relayed_sems.at[chunk, side],
            (down, up)[side],
        )

    def far_step(chunk):
        rows = pl.ds(pl.multiple_of(chunk * part, part), part)
        with jax.named_scope("wait_peer"):
            peer_copy(chunk).wait_recv()
        both = jnp.concatenate([stacked(state[levels, rows]), stacked(peer_state[rows])], axis=1)
        for slot in range(ring):
            with jax.named_scope(f"far{slot}"):
                value = product(both, expand_high[slot], expand_low[slot])
                share[chunk, slot, 0] = value[:, :half]
                share[chunk, slot, 1] = value[:, half:]
            if slot == 0:
                first_copy(chunk, 0).start()
                first_copy(chunk, 1).start()
            if slot == 1:
                straight_copy(chunk, 0).start()
            if slot == 2:
                straight_copy(chunk, 1).start()

    def relay_step(chunk):
        for side in range(2):
            with jax.named_scope("wait_first"):
                first_copy(chunk, side).wait_recv()
            share[chunk, 1 + side, side] = share[chunk, 1 + side, side] + first[chunk, side]
            relayed_copy(chunk, side).start()

    def near_ready(which):
        with jax.named_scope(f"wait_x{which}"):
            if which == 1:
                pl.when(has_before)(x_after.wait_recv)
            else:
                pl.when(has_after)(x_before.wait_recv)
        x_both[which] = stacked(x[which] * mask[0, which - 1].astype(F32))
        near_part(which)

    def main_body(step, carry):
        @pl.when(step < PARTS)
        def _():
            level_step(levels - 1, step)
            peer_copy(step).start()

        @pl.when(step >= 1)
        def _():
            far_step(step - 1)

        return carry

    lax.fori_loop(0, PARTS + 1, main_body, 0)

    relay_step(0)
    with jax.named_scope("g_fill"):
        g_span(FILLS[2], FILLS[3])
    relay_step(1)
    near_part(0)
    relay_step(2)
    near_ready(1)
    relay_step(3)
    near_ready(2)

    def final_body(chunk, carry):
        rows = pl.ds(pl.multiple_of(chunk * part, part), part)
        for side in range(2):
            with jax.named_scope("wait_relayed"):
                relayed_copy(chunk, side).wait_recv()
            span = pl.ds(side * half, half)
            out[rows, span] = (
                near[rows, span]
                + share[chunk, 3, side]
                + straight[chunk, 1 - side]
                + relayed[chunk, side]
            )
        return carry

    with jax.named_scope("wait_straight"):
        remote(straight, straight, sent_sems.at[levels + 1], straight_sem, up).wait_recv()
    lax.fori_loop(0, PARTS, final_body, 0)

    with jax.named_scope("drain"):
        for level in range(levels):
            remote(
                state.at[level], moved.at[level], sent_sems.at[level], level_sems.at[level, 0], up
            ).wait_send()
        remote(state.at[levels], peer_state, sent_sems.at[levels], peer_sems.at[0], up).wait_send()
        away = share.at[:, pl.ds(0, 3)]
        remote(away, away, sent_sems.at[levels + 1], straight_sem, up).wait_send()
        whole_expand.wait_send()
        for copy in (to_after, x_after):
            pl.when(has_after)(copy.wait_send)
        for copy in (to_before, x_before):
            pl.when(has_before)(copy.wait_send)


def order_kernel(order, number):
    number[0] = order[0] * 2 + (order[1] > order[2]).astype(jnp.int32)


def order_number(order):
    smem = pl.BlockSpec(memory_space=pltpu.SMEM)
    return pl.pallas_call(
        order_kernel,
        out_shape=jax.ShapeDtypeStruct((1,), jnp.int32),
        in_specs=[smem],
        out_specs=smem,
        name="order_number",
    )(order)


def solution(mesh):
    sizes = (mesh.shape["grp"], mesh.shape["node"])

    def shards(excitation, points, near_mask, bit_order, compress, level_self, level_partner, expand):
        cols, block = excitation.shape
        rank = compress.shape[1]
        levels = level_self.shape[0]
        part = cols // PARTS
        half = block // 2
        ring = sizes[0] // 2
        hbm = pl.BlockSpec(memory_space=pltpu.HBM)
        dma = pltpu.SemaphoreType.DMA

        def call(bits, number):
            return pl.pallas_call(
                functools.partial(kernel, bits, sizes),
                out_shape=jax.ShapeDtypeStruct((cols, block), F32),
                in_specs=[hbm] * 7,
                out_specs=pl.BlockSpec(memory_space=pltpu.VMEM),
                scratch_shapes=[
                    pltpu.SMEM((1, 2), jnp.int32),
                    pltpu.VMEM((3, cols, block), F32),
                    pltpu.VMEM((3, 3, block), F32),
                    pltpu.VMEM((3 * block, 8), F32),
                    pltpu.VMEM((3, 8, block), F32),
                    pltpu.VMEM((block, rank), F32),
                    pltpu.VMEM((2, levels, rank, rank), F32),
                    pltpu.VMEM((2, levels, rank, rank), BF16),
                    pltpu.VMEM((2, levels, rank, rank), BF16),
                    pltpu.VMEM((ring, 2 * rank, block), F32),
                    pltpu.VMEM((ring, 2 * rank, block), BF16),
                    pltpu.VMEM((ring, 2 * rank, block), BF16),
                    pltpu.VMEM((3 * block, block), BF16),
                    pltpu.VMEM((3 * block, block), BF16),
                    pltpu.VMEM((3, 2 * cols, block), BF16),
                    pltpu.VMEM((cols, block), F32),
                    pltpu.VMEM((levels + 1, cols, rank), F32),
                    pltpu.VMEM((levels, cols, rank), F32),
                    pltpu.VMEM((cols, rank), F32),
                    pltpu.VMEM((PARTS, ring, 2, part, half), F32),
                    pltpu.VMEM((PARTS, 2, part, half), F32),
                    pltpu.VMEM((PARTS, 2, part, half), F32),
                    pltpu.VMEM((PARTS, 2, part, half), F32),
                    dma((5,)),
                    dma,
                    dma((levels + 2,)),
                    dma((levels, PARTS)),
                    dma((PARTS,)),
                    dma((2,)),
                    dma((2, 2)),
                    dma((2, 2)),
                    dma((PARTS, 2)),
                    dma,
                    dma((PARTS, 2)),
                ],
                compiler_params=pltpu.CompilerParams(
                    collective_id=number, has_side_effects=True, vmem_limit_bytes=62 << 20
                ),
                name=f"far_near_{number}",
            )

        orders = list(itertools.permutations(range(levels)))
        branches = [call(bits, number) for number, bits in enumerate(orders)]
        return lax.switch(
            order_number(bit_order)[0],
            branches,
            excitation,
            points,
            near_mask,
            compress,
            level_self,
            level_partner,
            expand,
        )

    return jax.shard_map(
        shards,
        mesh=mesh,
        in_specs=(
            P(None, ("grp", "node")),
            P(None, ("grp", "node")),
            P(("grp", "node"), None),
            P(),
            P(("grp", "node"), None),
            P(None, ("grp", "node"), None),
            P(None, ("grp", "node"), None),
            P(("grp", "node"), None),
        ),
        out_specs=P(None, ("grp", "node")),
        check_vma=False,
    )
```

```python
import functools
import itertools

import jax
import jax.numpy as jnp
from jax import lax
from jax.experimental import pallas as pl
from jax.experimental.pallas import tpu as pltpu
from jax.sharding import PartitionSpec as P

F32 = jnp.float32
BF16 = jnp.bfloat16
MESH = pl.DeviceIdType.MESH
SOFTEN = 0.01

TALL = 64
AHEAD = 12
FILLS = (10, 20, 25, 38, 48)
PIECES = 2
PARTS = 4
AWAY = (2, 3, 1, 0)


def split(value):
    high = value.astype(BF16)
    return high, (value - high.astype(F32)).astype(BF16)


def product(left, right_high, right_low):
    rows = left.shape[0] // 2
    both = jnp.dot(left, right_high, preferred_element_type=F32)
    rest = jnp.dot(left[:rows], right_low, preferred_element_type=F32)
    return both[:rows] + both[rows:] + rest


def stacked(value):
    return jnp.concatenate(split(value), axis=0)


def remote(source, target, sends, receives, device):
    return pltpu.make_async_remote_copy(
        src_ref=source,
        dst_ref=target,
        send_sem=sends,
        recv_sem=receives,
        device_id=device,
        device_id_type=MESH,
    )


def kernel(
    bits,
    sizes,
    x_hbm,
    points_hbm,
    mask_hbm,
    compress_hbm,
    self_hbm,
    partner_hbm,
    expand_hbm,
    out,
    mask,
    x,
    points,
    columns,
    spread,
    compress,
    weights,
    weights_high,
    weights_low,
    expand,
    expand_high,
    expand_low,
    g_high,
    g_low,
    x_both,
    near,
    state,
    moved,
    peer_state,
    share,
    first,
    straight,
    relayed,
    load_sem,
    first_sem,
    expand_sem,
    sent_sems,
    level_sems,
    peer_sems,
    peer_expand_sems,
    points_sems,
    x_sems,
    first_sems,
    straight_sem,
    relayed_sems,
):
    n_grp, n_node = sizes
    levels = len(bits)
    cols, block = x_hbm.shape
    rank = compress_hbm.shape[1]
    part = cols // PARTS
    half = block // 2
    ring = n_grp // 2

    grp, node = lax.axis_index("grp"), lax.axis_index("node")
    y, core = lax.div(grp, 2), lax.rem(grp, 2)

    def along(step):
        return (lax.rem(y + step, ring) * 2 + core, node)

    up, down = along(1), along(ring - 1)
    peer = (grp + 1 - 2 * core, node)
    after, before = (grp, node + 1), (grp, node - 1)

    def partner(bit):
        apart = 1 << bit
        return (grp, node + apart * (1 - 2 * lax.rem(lax.div(node, apart), 2)))

    partners = [partner(bit) for bit in bits]
    has_before, has_after = node > 0, node < n_node - 1

    deep = block // PIECES

    def depth(piece):
        return pl.ds(piece * deep, deep)

    first_loads = [
        (
            pltpu.make_async_copy(x_hbm.at[:, depth(piece)], x.at[0, :, depth(piece)], first_sem.at[piece]),
            pltpu.make_async_copy(compress_hbm.at[depth(piece)], compress.at[depth(piece)], first_sem.at[PIECES + piece]),
        )
        for piece in range(PIECES)
    ]
    for pair in first_loads:
        for load in pair:
            load.start()
    loads = [
        pltpu.make_async_copy(points_hbm, points.at[0], load_sem.at[0]),
        pltpu.make_async_copy(mask_hbm, mask, load_sem.at[1]),
        pltpu.make_async_copy(self_hbm, weights.at[0], load_sem.at[2]),
        pltpu.make_async_copy(partner_hbm, weights.at[1], load_sem.at[2]),
    ]
    barrier = pltpu.get_barrier_semaphore()

    def greet(device):
        pl.semaphore_signal(barrier, inc=1, device_id=device, device_id_type=MESH)

    everyone = partners + [peer, up, down]
    for device in everyone:
        greet(device)

    @pl.when(has_before)
    def _():
        greet(before)

    @pl.when(has_after)
    def _():
        greet(after)


    def expand_columns(slot, of_core):
        target = lax.rem(y + AWAY[slot], ring) * 2 + of_core
        return expand_hbm.at[:, pl.ds(pl.multiple_of(target * block, block), block)]

    own_expand = [
        pltpu.make_async_copy(expand_columns(slot, core), expand.at[slot, pl.ds(0, rank)], expand_sem)
        for slot in range(ring)
    ]

    total = None
    for piece in range(PIECES):
        with jax.named_scope("load_x"):
            for load in first_loads[piece]:
                load.wait()
        if piece == 0:
            for load in loads:
                load.start()
        with jax.named_scope("compress"):
            value = stacked(x[0, :, depth(piece)])
            x_both[0, :, depth(piece)] = value
            value = product(value, *split(compress[depth(piece), :]))
            total = value if total is None else total + value
    state[0] = total
    for copy in own_expand:
        copy.start()

    with jax.named_scope("barrier"):
        pl.semaphore_wait(barrier, len(everyone) + has_before.astype(jnp.int32) + has_after.astype(jnp.int32))

    def level_copy(level, chunk):
        rows = pl.ds(pl.multiple_of(chunk * part, part), part)
        return remote(
            state.at[level, rows],
            moved.at[level, rows],
            sent_sems.at[level],
            level_sems.at[level, chunk],
            partners[level],
        )

    for chunk in range(PARTS):
        level_copy(0, chunk).start()

    loads[0].wait()
    to_after = remote(points.at[0], points.at[1], points_sems.at[0, 0], points_sems.at[1, 0], after)
    to_before = remote(points.at[0], points.at[2], points_sems.at[0, 1], points_sems.at[1, 1], before)

    @pl.when(has_after)
    def _():
        to_after.start()

    @pl.when(has_before)
    def _():
        to_before.start()

    @pl.when(jnp.logical_not(has_before))
    def _():
        points[1] = jnp.zeros_like(points[1])
        x[1] = jnp.zeros_like(x[1])

    @pl.when(jnp.logical_not(has_after))
    def _():
        points[2] = jnp.zeros_like(points[2])
        x[2] = jnp.zeros_like(x[2])

    peer_expand = [
        remote(
            expand_columns(slot, 1 - core),
            expand.at[slot, pl.ds(rank, rank)],
            peer_expand_sems.at[0],
            peer_expand_sems.at[1],
            peer,
        )
        for slot in range(ring)
    ]
    for copy in peer_expand:
        copy.start()

    with jax.named_scope("split_w"):
        loads[1].wait()
        pltpu.make_async_copy(weights, weights, load_sem.at[2]).wait()
        for level in range(levels):
            for which in range(2):
                high, low = split(weights[which, level])
                weights_high[which, level] = high
                weights_low[which, level] = low

    def turn(which):
        padded = jnp.concatenate([points[which] * 32.0, jnp.zeros((5, block), F32)], axis=0)
        columns[pl.ds(which * block, block), :] = padded.T

    def g_rows(index):
        for piece in range(TALL // 16):
            rows = pl.ds(pl.multiple_of(index * TALL + piece * 16, 16), 16)
            column = columns[rows, :]
            for side in range(2):
                span = pl.ds(side * half, half)
                total = None
                for axis in range(3):
                    source = jnp.broadcast_to(column[:, axis : axis + 1], (16, half))
                    target = jnp.concatenate([spread[axis, :, span]] * 2, axis=0)
                    apart = source - target
                    total = apart * apart if total is None else total + apart * apart
                high, low = split(lax.rsqrt(total + SOFTEN * 1024.0))
                g_high[rows, span] = high
                g_low[rows, span] = low

    wide = block // TALL

    def g_span(low, high):
        def body(index, carry):
            g_rows(index)
            return carry

        lax.fori_loop(low, high, body, 0)

    def near_part(which):
        def near_body(index, carry):
            span = pl.ds(pl.multiple_of(index * 512, 512), 512)
            rows = pl.ds(which * block, block)
            term = product(x_both[which], g_high[rows, span], g_low[rows, span])
            near[:, span] = term if which == 0 else near[:, span] + term
            return carry

        with jax.named_scope(f"near{which}"):
            lax.fori_loop(0, block // 512, near_body, 0)

    with jax.named_scope("turn0"):
        for axis in range(3):
            spread[axis] = jnp.broadcast_to(points[0, axis : axis + 1, :] * 32.0, (8, block))
        turn(0)
    with jax.named_scope("g_own"):
        g_span(0, FILLS[0])

    def level_step(level, chunk):
        rows = pl.ds(pl.multiple_of(chunk * part, part), part)
        with jax.named_scope(f"own{level}"):
            own = product(stacked(state[level, rows]), weights_high[0, level], weights_low[0, level])
        with jax.named_scope(f"wait{level}"):
            level_copy(level, chunk).wait_recv()
        with jax.named_scope(f"came{level}"):
            came = product(stacked(moved[level, rows]), weights_high[1, level], weights_low[1, level])
            state[level + 1, rows] = own + came

    for level in range(levels - 1):

        def level_body(chunk, carry, level=level):
            level_step(level, chunk)
            level_copy(level + 1, chunk).start()
            return carry

        lax.fori_loop(0, PARTS, level_body, 0)
        if level == 0:
            with jax.named_scope("turn12"):
                pl.when(has_before)(to_after.wait_recv)
                pl.when(has_after)(to_before.wait_recv)
                turn(1)
                turn(2)
            with jax.named_scope("g_1"):
                g_span(FILLS[0], FILLS[1])

    x_after = remote(x.at[0], x.at[1], x_sems.at[0, 0], x_sems.at[1, 0], after)
    x_before = remote(x.at[0], x.at[2], x_sems.at[0, 1], x_sems.at[1, 1], before)
    pl.when(has_after)(x_after.start)
    pl.when(has_before)(x_before.start)

    whole_expand = remote(
        expand.at[:, pl.ds(0, rank)],
        expand.at[:, pl.ds(rank, rank)],
        peer_expand_sems.at[0],
        peer_expand_sems.at[1],
        peer,
    )
    with jax.named_scope("wait_e"):
        pltpu.make_async_copy(
            expand.at[:, pl.ds(0, rank)], expand.at[:, pl.ds(0, rank)], expand_sem
        ).wait()
        whole_expand.wait_recv()
    for slot in range(ring):

        def convert(index, carry, slot=slot):
            rows = pl.ds(pl.multiple_of(index * 32, 32), 32)
            high, low = split(expand[slot, rows, :])
            expand_high[slot, rows, :] = high
            expand_low[slot, rows, :] = low
            return carry

        with jax.named_scope("convert"):
            lax.fori_loop(0, rank // 16, convert, 0)

    with jax.named_scope("g_2"):
        g_span(FILLS[1], FILLS[2])

    def peer_copy(chunk):
        rows = pl.ds(pl.multiple_of(chunk * part, part), part)
        return remote(
            state.at[levels, rows],
            peer_state.at[rows],
            sent_sems.at[levels],
            peer_sems.at[chunk],
            peer,
        )

    def first_copy(chunk, side):
        return remote(
            share.at[chunk, 0, side],
            first.at[chunk, side],
            sent_sems.at[levels + 1],
            first_sems.at[chunk],
            (down, up)[side],
        )

    def straight_copy(chunk, side):
        return remote(
            share.at[chunk, 1 + side, 1 - side],
            straight.at[chunk, side],
            sent_sems.at[levels + 1],
            straight_sem,
            (down, up)[side],
        )

    def relayed_copy(chunk, side):
        return remote(
            share.at[chunk, 1 + side, side],
            relayed.at[chunk, side],
            sent_sems.at[levels + 1],
            relayed_sems.at[chunk],
            (down, up)[side],
        )

    def far_step(chunk):
        rows = pl.ds(pl.multiple_of(chunk * part, part), part)
        with jax.named_scope("wait_peer"):
            peer_copy(chunk).wait_recv()
        both = jnp.concatenate([stacked(state[levels, rows]), stacked(peer_state[rows])], axis=1)
        def far_slot(slot, carry):
            with jax.named_scope("far"):
                value = product(both, expand_high[slot], expand_low[slot])
                share[chunk, slot, 0] = value[:, :half]
                share[chunk, slot, 1] = value[:, half:]

            @pl.when(slot == 0)
            def _():
                first_copy(chunk, 0).start()
                first_copy(chunk, 1).start()

            @pl.when(slot == 1)
            def _():
                straight_copy(chunk, 0).start()

            @pl.when(slot == 2)
            def _():
                straight_copy(chunk, 1).start()

            return carry

        lax.fori_loop(0, ring, far_slot, 0)

    def relay_step(chunk):
        with jax.named_scope("wait_first"):
            both = first.at[chunk]
            remote(both, both, sent_sems.at[levels + 1], first_sems.at[chunk], up).wait_recv()
        for side in range(2):
            share[chunk, 1 + side, side] = share[chunk, 1 + side, side] + first[chunk, side]
            relayed_copy(chunk, side).start()

    def near_ready(which):
        with jax.named_scope(f"wait_x{which}"):
            if which == 1:
                pl.when(has_before)(x_after.wait_recv)
            else:
                pl.when(has_after)(x_before.wait_recv)
        x_both[which] = stacked(x[which] * mask[0, which - 1].astype(F32))
        near_part(which)

    def last_level(chunk, carry=0):
        level_step(levels - 1, chunk)
        peer_copy(chunk).start()
        return carry

    lax.fori_loop(0, 1 + (PARTS - 1) * core, last_level, 0)

    begun = FILLS[2] + AHEAD * core
    with jax.named_scope("g_ahead"):
        g_span(FILLS[2], begun)

    def main_body(chunk, carry):
        far_step(chunk)

        @pl.when(jnp.logical_and(core == 0, chunk < PARTS - 1))
        def _():
            last_level(chunk + 1)

        return carry

    lax.fori_loop(0, PARTS, main_body, 0)

    relay_step(0)
    with jax.named_scope("g_fill"):
        g_span(begun, FILLS[3])
    relay_step(1)
    with jax.named_scope("g_fill"):
        g_span(FILLS[3], FILLS[4])
    relay_step(2)
    near_part(0)
    relay_step(3)
    near_ready(1)
    near_ready(2)

    def final_body(chunk, carry):
        rows = pl.ds(pl.multiple_of(chunk * part, part), part)
        with jax.named_scope("wait_relayed"):
            both = relayed.at[chunk]
            remote(both, both, sent_sems.at[levels + 1], relayed_sems.at[chunk], up).wait_recv()
        for side in range(2):
            span = pl.ds(side * half, half)
            out[rows, span] = (
                near[rows, span]
                + share[chunk, 3, side]
                + straight[chunk, 1 - side]
                + relayed[chunk, side]
            )
        return carry

    with jax.named_scope("wait_straight"):
        remote(straight, straight, sent_sems.at[levels + 1], straight_sem, up).wait_recv()
    lax.fori_loop(0, PARTS, final_body, 0)

    with jax.named_scope("drain"):
        for level in range(levels):
            remote(
                state.at[level], moved.at[level], sent_sems.at[level], level_sems.at[level, 0], up
            ).wait_send()
        remote(state.at[levels], peer_state, sent_sems.at[levels], peer_sems.at[0], up).wait_send()
        away = share.at[:, pl.ds(0, 3)]
        remote(away, away, sent_sems.at[levels + 1], straight_sem, up).wait_send()
        whole_expand.wait_send()
        for copy in (to_after, x_after):
            pl.when(has_after)(copy.wait_send)
        for copy in (to_before, x_before):
            pl.when(has_before)(copy.wait_send)


def order_kernel(order, number):
    number[0] = order[0] * 2 + (order[1] > order[2]).astype(jnp.int32)


def order_number(order):
    smem = pl.BlockSpec(memory_space=pltpu.SMEM)
    return pl.pallas_call(
        order_kernel,
        out_shape=jax.ShapeDtypeStruct((1,), jnp.int32),
        in_specs=[smem],
        out_specs=smem,
        name="order_number",
    )(order)


def solution(mesh):
    sizes = (mesh.shape["grp"], mesh.shape["node"])

    def shards(excitation, points, near_mask, bit_order, compress, level_self, level_partner, expand):
        cols, block = excitation.shape
        rank = compress.shape[1]
        levels = level_self.shape[0]
        part = cols // PARTS
        half = block // 2
        ring = sizes[0] // 2
        hbm = pl.BlockSpec(memory_space=pltpu.HBM)
        dma = pltpu.SemaphoreType.DMA

        def call(bits, number):
            return pl.pallas_call(
                functools.partial(kernel, bits, sizes),
                out_shape=jax.ShapeDtypeStruct((cols, block), F32),
                in_specs=[hbm] * 7,
                out_specs=pl.BlockSpec(memory_space=pltpu.VMEM),
                scratch_shapes=[
                    pltpu.SMEM((1, 2), jnp.int32),
                    pltpu.VMEM((3, cols, block), F32),
                    pltpu.VMEM((3, 3, block), F32),
                    pltpu.VMEM((3 * block, 8), F32),
                    pltpu.VMEM((3, 8, block), F32),
                    pltpu.VMEM((block, rank), F32),
                    pltpu.VMEM((2, levels, rank, rank), F32),
                    pltpu.VMEM((2, levels, rank, rank), BF16),
                    pltpu.VMEM((2, levels, rank, rank), BF16),
                    pltpu.VMEM((ring, 2 * rank, block), F32),
                    pltpu.VMEM((ring, 2 * rank, block), BF16),
                    pltpu.VMEM((ring, 2 * rank, block), BF16),
                    pltpu.VMEM((3 * block, block), BF16),
                    pltpu.VMEM((3 * block, block), BF16),
                    pltpu.VMEM((3, 2 * cols, block), BF16),
                    pltpu.VMEM((cols, block), F32),
                    pltpu.VMEM((levels + 1, cols, rank), F32),
                    pltpu.VMEM((levels, cols, rank), F32),
                    pltpu.VMEM((cols, rank), F32),
                    pltpu.VMEM((PARTS, ring, 2, part, half), F32),
                    pltpu.VMEM((PARTS, 2, part, half), F32),
                    pltpu.VMEM((PARTS, 2, part, half), F32),
                    pltpu.VMEM((PARTS, 2, part, half), F32),
                    dma((3,)),
                    dma((2 * PIECES,)),
                    dma,
                    dma((levels + 2,)),
                    dma((levels, PARTS)),
                    dma((PARTS,)),
                    dma((2,)),
                    dma((2, 2)),
                    dma((2, 2)),
                    dma((PARTS,)),
                    dma,
                    dma((PARTS,)),
                ],
                compiler_params=pltpu.CompilerParams(
                    collective_id=number, has_side_effects=True, vmem_limit_bytes=62 << 20
                ),
                name=f"far_near_{number}",
            )

        orders = list(itertools.permutations(range(levels)))
        branches = [call(bits, number) for number, bits in enumerate(orders)]
        return lax.switch(
            order_number(bit_order)[0],
            branches,
            excitation,
            points,
            near_mask,
            compress,
            level_self,
            level_partner,
            expand,
        )

    return jax.shard_map(
        shards,
        mesh=mesh,
        in_specs=(
            P(None, ("grp", "node")),
            P(None, ("grp", "node")),
            P(("grp", "node"), None),
            P(),
            P(("grp", "node"), None),
            P(None, ("grp", "node"), None),
            P(None, ("grp", "node"), None),
            P(("grp", "node"), None),
        ),
        out_specs=P(None, ("grp", "node")),
        check_vma=False,
    )
```
